16 devices in a mesh: tp: 2 (over z), ep: 8 (over y, x, core).
Axes of the slice: x: 2, y: 2, z: 2, core: 2. Of those that a mesh axis runs over, the one named last changes fastest.
Arguments:
- x_norm: bfloat16 [8192, 1024], P(('ep', 'tp'))
- route_idx: int32 [8192, 8], P(('ep', 'tp'))
- route_slot: int32 [8192, 8], P(('ep', 'tp'))
- w_router: bfloat16 [1024, 32], replicated
- b_router: float32 [32], replicated
- w_gate_up: bfloat16 [32, 1024, 1024], P('ep', None, 'tp')
- b_gate_up: float32 [32, 1024], P('ep', 'tp')
- w_down: bfloat16 [32, 512, 1024], P('ep', 'tp')
- b_down: float32 [32, 1024], P('ep')
- d_out: bfloat16 [8192, 1024], P(('ep', 'tp'))
Outputs:
- output 1: bfloat16 [8192, 1024], P(('ep', 'tp'))
- output 2: bfloat16 [8192, 1024], P(('ep', 'tp'))
- output 3: bfloat16 [32, 1024, 1024], P('ep', None, 'tp')
- output 4: float32 [32, 1024], P('ep', 'tp')
- output 5: bfloat16 [32, 512, 1024], P('ep', 'tp')
- output 6: float32 [32, 1024], P('ep')
- output 7: float32 [1024, 32], replicated
- output 8: float32 [32], replicated
All inputs are finite; a program needn't handle non-finite values.
Results may differ from the reference program's by a relative error of at most 0.0122586.
Values are sent between devices in bfloat16 or wider.
A program may use at most 1 GiB of HBM per device.

```python
import functools
import jax
import jax.numpy as jnp
from jax import lax

HIDDEN = 1024
EXPERT_WIDTH = 512
EXPERTS = 32
TOP_K = 8
TOK_DEV = 512
DEVICES = 16
TP_SIZE = 2
TOKENS = TOK_DEV * DEVICES
CAPACITY = 2 * TOK_DEV * TOP_K // EXPERTS
SHARD_WIDTH = EXPERT_WIDTH // TP_SIZE
HOT_COUNT = max(1, EXPERTS // 8)
BUF_ROWS = EXPERTS * DEVICES * CAPACITY
CLAMP_LIMIT = 7.0
SWIGLU_ALPHA = 1.702


def draw_routing(route_key):
    perm_key, score_key = jax.random.split(route_key)
    hot_order = jax.random.permutation(perm_key, EXPERTS)
    hot_bonus = jnp.zeros((EXPERTS,), jnp.int32).at[hot_order[:HOT_COUNT]].set(32)
    scores = jax.random.randint(score_key, (TOKENS, EXPERTS), 0, 256, jnp.int32) + hot_bonus[None, :]
    local_pos = jnp.arange(TOKENS) % TOK_DEV
    forced = (local_pos < 2 * CAPACITY)[:, None] & (jnp.arange(EXPERTS) == hot_order[0])[None, :]
    scores = jnp.where(forced, 4096, scores)
    keyed_scores = scores * EXPERTS + jnp.arange(EXPERTS, dtype=jnp.int32)[None, :]
    route_idx = lax.top_k(keyed_scores, TOP_K)[1]
    expert_hits = (route_idx[:, :, None] == jnp.arange(EXPERTS)[None, None, :]).astype(jnp.int32)
    expert_hits = expert_hits.reshape(DEVICES, TOK_DEV * TOP_K, EXPERTS)
    slot_rank = jnp.sum((jnp.cumsum(expert_hits, axis=1) - 1) * expert_hits, axis=2)
    slot_rank = slot_rank.reshape(TOKENS, TOP_K)
    route_slot = jnp.where(slot_rank < CAPACITY, slot_rank, -1)
    return route_idx.astype(jnp.int32), route_slot.astype(jnp.int32)


def setup_inputs(seed: int = 0) -> dict:
    base_key = jax.random.key(seed)
    sub_keys = jax.random.split(base_key, 9)
    x_norm = jax.random.normal(sub_keys[0], (TOKENS, HIDDEN), jnp.float32)
    w_router = jax.random.normal(sub_keys[1], (HIDDEN, EXPERTS), jnp.float32) * HIDDEN ** -0.5
    b_router = jax.random.normal(sub_keys[2], (EXPERTS,), jnp.float32)
    w_gate_up = jax.random.normal(sub_keys[3], (EXPERTS, HIDDEN, 2 * EXPERT_WIDTH), jnp.float32) * (3.0 * HIDDEN ** -0.5)
    b_gate_up = jax.random.normal(sub_keys[4], (EXPERTS, 2 * EXPERT_WIDTH), jnp.float32)
    w_down = jax.random.normal(sub_keys[5], (EXPERTS, EXPERT_WIDTH, HIDDEN), jnp.float32) * (0.25 * EXPERT_WIDTH ** -0.5)
    b_down = jax.random.normal(sub_keys[6], (EXPERTS, HIDDEN), jnp.float32)
    d_out = jax.random.normal(sub_keys[7], (TOKENS, HIDDEN), jnp.float32)
    route_idx, route_slot = draw_routing(sub_keys[8])
    return {'x_norm': x_norm.astype(jnp.bfloat16), 'route_idx': route_idx, 'route_slot': route_slot, 'w_router': w_router.astype(jnp.bfloat16), 'b_router': b_router, 'w_gate_up': w_gate_up.astype(jnp.bfloat16), 'b_gate_up': b_gate_up, 'w_down': w_down.astype(jnp.bfloat16), 'b_down': b_down, 'd_out': d_out.astype(jnp.bfloat16)}


def bf16_snap(value):
    return value + lax.stop_gradient(value.astype(jnp.bfloat16).astype(jnp.float32) - value)


def clamped_swiglu(h_pair):
    gate_val = jnp.minimum(h_pair[..., 0], CLAMP_LIMIT)
    up_val = jnp.clip(h_pair[..., 1], -CLAMP_LIMIT, CLAMP_LIMIT)
    return gate_val * jax.nn.sigmoid(SWIGLU_ALPHA * gate_val) * (up_val + 1.0)


def expert_rows(operands):
    rows_in, w_gu_one, b_gu_one, w_dn_one, b_dn_one = operands
    hidden_pre = jnp.dot(rows_in, w_gu_one) + b_gu_one[None, :]
    act_val = bf16_snap(clamped_swiglu(hidden_pre.reshape(-1, EXPERT_WIDTH, 2)))
    part_out = jnp.einsum('rsf,sfd->rsd', act_val.reshape(-1, TP_SIZE, SHARD_WIDTH), w_dn_one.reshape(TP_SIZE, SHARD_WIDTH, HIDDEN))
    first_mask = (jnp.arange(TP_SIZE) == 0).astype(part_out.dtype)
    part_out = bf16_snap(part_out + first_mask[None, :, None] * b_dn_one[None, None, :])
    return bf16_snap(jnp.sum(part_out, axis=1))


def block_forward(x_wide, w_router, b_router, w_gate_up, b_gate_up, w_down, b_down, route_idx, route_slot):
    logits = jnp.dot(x_wide, w_router) + b_router[None, :]
    gate_w = jax.nn.softmax(jnp.take_along_axis(logits, route_idx, axis=1), axis=1)
    is_kept = route_slot >= 0
    source_dev = (jnp.arange(TOKENS) // TOK_DEV)[:, None]
    flat_pos = jnp.where(is_kept, (route_idx * DEVICES + source_dev) * CAPACITY + route_slot, BUF_ROWS)
    token_ids = jnp.broadcast_to(jnp.arange(TOKENS, dtype=jnp.int32)[:, None], (TOKENS, TOP_K))
    row_token = jnp.full((BUF_ROWS,), TOKENS, jnp.int32).at[flat_pos.reshape(-1)].set(token_ids.reshape(-1), mode='drop')
    x_pad = jnp.concatenate([x_wide, jnp.zeros((1, HIDDEN), x_wide.dtype)], axis=0)
    routed_rows = x_pad[row_token].reshape(EXPERTS, DEVICES * CAPACITY, HIDDEN)
    expert_out = lax.map(jax.checkpoint(expert_rows), (routed_rows, w_gate_up, b_gate_up, w_down, b_down))
    y_flat = expert_out.reshape(BUF_ROWS, HIDDEN)
    safe_pos = jnp.where(is_kept, flat_pos, 0)
    kept_w = gate_w * is_kept.astype(gate_w.dtype)
    moe_acc = jnp.zeros((TOKENS, HIDDEN), gate_w.dtype)
    for choice in range(TOP_K):
        moe_acc = moe_acc + kept_w[:, choice:choice + 1] * y_flat[safe_pos[:, choice]]
    return bf16_snap(moe_acc)


def reference(x_norm, route_idx, route_slot, w_router, b_router, w_gate_up, b_gate_up, w_down, b_down, d_out):
    forward_fn = functools.partial(block_forward, route_idx=route_idx, route_slot=route_slot)
    moe_out, pullback = jax.vjp(forward_fn, x_norm.astype(jnp.float32), w_router.astype(jnp.float32), b_router, w_gate_up.astype(jnp.float32), b_gate_up, w_down.astype(jnp.float32), b_down)
    grad_all = pullback(d_out.astype(jnp.float32))
    return (moe_out.astype(jnp.bfloat16), grad_all[0].astype(jnp.bfloat16), grad_all[3].astype(jnp.bfloat16), grad_all[4], grad_all[5].astype(jnp.bfloat16), grad_all[6], grad_all[1], grad_all[2])
```

```python
import functools

import jax
import jax.numpy as jnp
from jax import lax
from jax.experimental import pallas as pl
from jax.experimental.pallas import tpu as pltpu
from jax.sharding import PartitionSpec as P

CLAMP_LIMIT = 7.0
SWIGLU_ALPHA = 1.702
BF16 = jnp.bfloat16
F32 = jnp.float32
ORDER = (0, 1, 8, 9, 4, 5, 2, 3, 12, 13, 6, 7, 10, 11, 14, 15)


def clamped_swiglu(gate_raw, up_raw):
    gate_val = jnp.minimum(gate_raw, CLAMP_LIMIT)
    up_val = jnp.clip(up_raw, -CLAMP_LIMIT, CLAMP_LIMIT)
    return gate_val * jax.nn.sigmoid(SWIGLU_ALPHA * gate_val) * (up_val + 1.0)


def dot32(lhs, rhs):
    return jnp.dot(lhs, rhs, preferred_element_type=F32)


def expert_kernel(n_blocks, n_exp, tok, dim, width, *refs):
    blocks = refs[:n_blocks]
    wgu_hbm, wgut_hbm, wd_hbm, wdt_hbm, bgu_ref, bd_ref, selrow_ref, selcol_ref = refs[n_blocks:n_blocks + 8]
    outs = refs[n_blocks + 8:2 * n_blocks + 8]
    dg_ref, gwgut_hbm, gwd_hbm, gbgu_ref, gbd_ref = refs[2 * n_blocks + 8:2 * n_blocks + 13]
    (xd, out_buf, moe_acc, dx_acc, wgu, wgut, wd, wdt, gwgut, gwd, xe_s, de_s, dc_s, p_s, dr_s,
     in_sem, out_sem, w_sem, g_sem) = refs[2 * n_blocks + 13:]
    meta_at = 2 * dim

    def load(i, buf):
        return pltpu.make_async_copy(blocks[i], xd.at[buf], in_sem.at[buf])

    def store(i, buf):
        return pltpu.make_async_copy(out_buf.at[buf], outs[i], out_sem.at[buf])

    def weights(e):
        return [pltpu.make_async_copy(src.at[e], dst.at[e], w_sem.at[k, e])
                for k, (src, dst) in enumerate(((wgu_hbm, wgu), (wgut_hbm, wgut), (wd_hbm, wd), (wdt_hbm, wdt)))]

    load(0, 0).start()
    for e in range(n_exp):
        for cp in weights(e):
            cp.start()
    gwgut[...] = jnp.zeros_like(gwgut)
    gwd[...] = jnp.zeros_like(gwd)
    gbgu_ref[...] = jnp.zeros_like(gbgu_ref)
    gbd_ref[...] = jnp.zeros_like(gbd_ref)

    def step(it, carry):
        g = it // n_exp
        e = it % n_exp
        buf = g % 2

        @pl.when(e == 0)
        def _():
            for i in range(n_blocks):
                @pl.when(g == i)
                def _():
                    load(i, i % 2).wait()
                    if i + 1 < n_blocks:
                        load(i + 1, (i + 1) % 2).start()
                    if i >= 2:
                        store(i - 2, i % 2).wait()
            moe_acc[...] = jnp.zeros_like(moe_acc)
            dx_acc[...] = jnp.zeros_like(dx_acc)

        @pl.when(g == 0)
        def _():
            for k in range(n_exp):
                @pl.when(e == k)
                def _():
                    for cp in weights(k):
                        cp.wait()

        meta = xd[buf, :, meta_at:meta_at + 128]
        rows = lax.dot_general(selrow_ref[e], meta, (((1,), (1,)), ((), ())), preferred_element_type=F32)
        slot_row = rows[0:1]
        w_row = rows[8:9]
        cols = dot32(meta, selcol_ref[e])
        slot_col = cols[:, :128].astype(jnp.int32)
        w_col = cols[:, 128:]
        count = jnp.max(slot_row)
        slot_i = slot_row.astype(jnp.int32)

        def tile(rows_t):
            hit = lax.broadcasted_iota(jnp.int32, (rows_t, tok), 0) == slot_i
            pick = jnp.where(hit, 1.0, 0.0).astype(BF16)
            w_slot = jnp.sum(jnp.where(hit, w_row, 0.0), axis=1, keepdims=True)
            sl = pl.ds(0, rows_t)
            for c in range(0, dim, 512):
                xe_s[sl, c:c + 512] = dot32(pick, xd[buf, :, c:c + 512]).astype(BF16)
            for c in range(0, dim, 512):
                d_rows = dot32(pick, xd[buf, :, dim + c:dim + c + 512])
                de_s[sl, c:c + 512] = d_rows
                dc_s[sl, c:c + 512] = (w_slot * d_rows).astype(BF16)
            hid = dot32(xe_s[sl, :], wgu[e]) + bgu_ref[e]
            act, pull = jax.vjp(clamped_swiglu, hid[:, :width], hid[:, width:])
            act_b = act.astype(BF16)
            dgs = jnp.zeros((rows_t, 1), F32)
            for c in range(0, dim, 512):
                part = (dot32(act_b, wd[e, :, c:c + 512]) + bd_ref[e, :, c:c + 512]).astype(BF16)
                p_s[sl, c:c + 512] = part
                dgs = dgs + jnp.sum(part.astype(F32) * de_s[sl, c:c + 512], axis=1, keepdims=True)
            dg_ref[it] = jnp.sum(jnp.where(hit, dgs, 0.0), axis=0, keepdims=True)
            d_act = dot32(dc_s[sl, :], wdt[e])
            d_gate, d_up = pull(d_act)
            d_hid = jnp.concatenate([d_gate, d_up], axis=1)
            gbgu_ref[e] += jnp.sum(d_hid, axis=0, keepdims=True)
            gbd_ref[e] += dot32(jnp.ones((16, rows_t), BF16), dc_s[sl, :])[0:1]
            d_hid_b = d_hid.astype(BF16)
            for c in range(0, dim, 512):
                dr_s[sl, c:c + 512] = dot32(d_hid_b, wgut[e, :, c:c + 512]).astype(BF16)
            act_t = act_b.T
            d_hid_t = d_hid_b.T
            for c in range(0, dim, 512):
                gwd[e, :, c:c + 512] += dot32(act_t, dc_s[sl, c:c + 512])
                gwgut[e, :, c:c + 512] += dot32(d_hid_t, xe_s[sl, c:c + 512])
            lane = lax.broadcasted_iota(jnp.int32, (tok, rows_t), 1)
            slot_wide = slot_col if rows_t == 128 else jnp.concatenate([slot_col] * (rows_t // 128), axis=1)
            place = jnp.where(lane == slot_wide, 1.0, 0.0).astype(BF16)
            w_wide = jnp.concatenate([w_col] * 4, axis=1)
            for c in range(0, dim, 512):
                moe_acc[:, c:c + 512] += w_wide * dot32(place, p_s[sl, c:c + 512])
                dx_acc[:, c:c + 512] += dot32(place, dr_s[sl, c:c + 512])

        @pl.when(count < 127.5)
        def _():
            tile(128)

        @pl.when(count > 127.5)
        def _():
            tile(256)

        @pl.when(e == n_exp - 1)
        def _():
            out_buf[buf, :, :dim] = moe_acc[...].astype(BF16)
            out_buf[buf, :, dim:] = dx_acc[...].astype(BF16)
            for i in range(n_blocks):
                @pl.when(g == i)
                def _():
                    store(i, i % 2).start()
        return carry

    lax.fori_loop(0, n_blocks * n_exp, step, 0)
    g_out = [pltpu.make_async_copy(gwgut, gwgut_hbm, g_sem.at[0]), pltpu.make_async_copy(gwd, gwd_hbm, g_sem.at[1])]
    for cp in g_out:
        cp.start()
    for i in range(max(0, n_blocks - 2), n_blocks):
        store(i, i % 2).wait()
    for cp in g_out:
        cp.wait()


def run_experts(blocks, wgu, wgut, wd, wdt, bgu, bd, selrow, selcol):
    n_blocks = len(blocks)
    n_exp, dim, two_w = wgu.shape
    width = two_w // 2
    tok, row_w = blocks[0].shape
    any_spec = pl.BlockSpec(memory_space=pl.ANY)
    vm_spec = pl.BlockSpec(memory_space=pltpu.VMEM)
    flops = n_blocks * n_exp * 2 * 128 * dim * (6 * tok + 6 * two_w)
    out = pl.pallas_call(
        functools.partial(expert_kernel, n_blocks, n_exp, tok, dim, width),
        out_shape=[jax.ShapeDtypeStruct((tok, 2 * dim), BF16)] * n_blocks + [
            jax.ShapeDtypeStruct((n_blocks * n_exp, 1, tok), F32),
            jax.ShapeDtypeStruct((n_exp, two_w, dim), F32),
            jax.ShapeDtypeStruct((n_exp, width, dim), F32),
            jax.ShapeDtypeStruct((n_exp, 1, two_w), F32),
            jax.ShapeDtypeStruct((n_exp, 1, dim), F32),
        ],
        in_specs=[any_spec] * (n_blocks + 4) + [vm_spec] * 4,
        out_specs=[any_spec] * n_blocks + [vm_spec, any_spec, any_spec, vm_spec, vm_spec],
        scratch_shapes=[
            pltpu.VMEM((2, tok, row_w), BF16),
            pltpu.VMEM((2, tok, 2 * dim), BF16),
            pltpu.VMEM((tok, dim), F32),
            pltpu.VMEM((tok, dim), F32),
            pltpu.VMEM((n_exp, dim, two_w), BF16),
            pltpu.VMEM((n_exp, two_w, dim), BF16),
            pltpu.VMEM((n_exp, width, dim), BF16),
            pltpu.VMEM((n_exp, dim, width), BF16),
            pltpu.VMEM((n_exp, two_w, dim), F32),
            pltpu.VMEM((n_exp, width, dim), F32),
            pltpu.VMEM((256, dim), BF16),
            pltpu.VMEM((256, dim), F32),
            pltpu.VMEM((256, dim), BF16),
            pltpu.VMEM((256, dim), BF16),
            pltpu.VMEM((256, dim), BF16),
            pltpu.SemaphoreType.DMA((2,)),
            pltpu.SemaphoreType.DMA((2,)),
            pltpu.SemaphoreType.DMA((4, n_exp)),
            pltpu.SemaphoreType.DMA((2,)),
        ],
        compiler_params=pltpu.CompilerParams(vmem_limit_bytes=60 * 1024 * 1024),
        cost_estimate=pl.CostEstimate(flops=flops, bytes_accessed=n_blocks * tok * 4 * dim * 2, transcendentals=0),
        name='experts',
    )(*blocks, wgu, wgut, wd, wdt, bgu, bd, selrow, selcol)
    return out[:n_blocks], out[n_blocks:]


def solution(mesh):
    tp_count = mesh.shape['tp']
    ep_count = mesh.shape['ep']
    n_dev = tp_count * ep_count
    tok_spec = P(('ep', 'tp'), None)
    axes = ('tp', 'ep')

    def flip(val, bit):
        return lax.ppermute(val, axes, [(i, i ^ bit) for i in range(n_dev)])

    def device_fn(x_loc, idx_loc, slot_loc, w_router, b_router, w_gate_up, b_gate_up, w_down, b_down, dy_loc):
        tok, dim = x_loc.shape
        n_experts = w_router.shape[1]
        n_exp = w_gate_up.shape[0]
        two_w = w_gate_up.shape[2]
        width = two_w // 2
        tp_index = lax.axis_index('tp')
        ep_index = lax.axis_index('ep')
        cut = (0, 176, 352, tok)

        logits = dot32(x_loc, w_router) + b_router[None, :]
        expert_hot = idx_loc[:, :, None] == jnp.arange(n_experts)[None, None, :]
        picked = jnp.sum(jnp.where(expert_hot, logits[:, None, :], 0.0), axis=2)
        gate_w = jax.nn.softmax(picked, axis=1)
        kept = jnp.any(expert_hot & (slot_loc >= 0)[:, :, None], axis=1)
        before = (jnp.arange(tok)[:, None] > jnp.arange(tok)[None, :]).astype(BF16)
        rank = dot32(before, kept.astype(BF16))
        slot_e = jnp.where(kept, rank, -1.0)
        w_e = jnp.sum(jnp.where(expert_hot, gate_w[:, :, None], 0.0), axis=1)
        w_hi = lax.reduce_precision(w_e, 8, 7)
        w_mid = lax.reduce_precision(w_e - w_hi, 8, 7)
        w_lo = w_e - w_hi - w_mid
        meta = jnp.concatenate([slot_e, w_hi, w_mid, w_lo], axis=1).astype(BF16)
        own = jnp.concatenate([x_loc, dy_loc, meta], axis=1)

        blk = {0: own}
        for bit in (8, 4, 2):
            blk[bit] = flip(own, bit)
        blk[12] = flip(blk[4], 8)
        blk[6] = flip(blk[2], 4)
        blk[10] = flip(blk[8], 2)
        far = ((6, 8), (10, 4), (12, 2))
        blk[14] = jnp.concatenate([flip(blk[m][cut[k]:cut[k + 1]], bit) for k, (m, bit) in enumerate(far)], axis=0)
        for m in range(0, 16, 2):
            blk[m + 1] = flip(blk[m], 1)

        col = jnp.arange(two_w)
        target = jnp.where(col % 2 == 0, col // 2, width + col // 2)
        perm = (target[:, None] == col[None, :]).astype(BF16)
        wgu = dot32(w_gate_up.reshape(n_exp * dim, two_w), perm).astype(BF16).reshape(n_exp, dim, two_w)
        wgut = jnp.swapaxes(wgu, 1, 2)
        wdt = jnp.swapaxes(w_down, 1, 2)
        bgu = b_gate_up.reshape(n_exp, width, 2)
        bgu = jnp.concatenate([bgu[:, :, 0], bgu[:, :, 1]], axis=1)[:, None, :]
        bias_on = (tp_index == 0).astype(F32)
        bd = (bias_on * b_down)[:, None, :]
        mine = ep_index * n_exp + jnp.arange(n_exp)
        lane = jnp.arange(128)
        sel_slot = lane[None, :] == mine[:, None]
        sel_w = (lane[None, :] % n_experts == mine[:, None]) & (lane[None, :] >= n_experts)
        row_id = jnp.arange(16)[None, :, None]
        selrow = jnp.where(row_id == 0, sel_slot[:, None, :], (row_id == 8) & sel_w[:, None, :]).astype(BF16)
        side = jnp.arange(256)[None, None, :] < 128
        selcol = jnp.where(side, sel_slot[:, :, None], sel_w[:, :, None]).astype(BF16)

        parts, (dg, gwgut, gwd, gbgu, gbd) = run_experts([blk[m] for m in ORDER], wgu, wgut, w_down, wdt, bgu, bd, selrow, selcol)
        part = dict(zip(ORDER, parts))

        lin = tp_index * ep_count + ep_index
        dg_abs = dg.reshape(n_dev, n_exp * tok)[jnp.array([ORDER.index(m) for m in range(n_dev)])][jnp.arange(n_dev) ^ lin]
        dg_back = lax.all_to_all(dg_abs, axes, 0, 0, tiled=True)
        dg_back = dg_back.reshape(tp_count, ep_count * n_exp, tok).sum(axis=0)
        d_gate_e = dg_back.T

        def wide(val):
            return val.astype(F32)

        acc = {m: (wide(part[m]) + wide(flip(part[m + 1], 1))).astype(BF16) for m in range(0, 16, 2)}
        for k, (m, bit) in enumerate(far):
            lo, hi = cut[k], cut[k + 1]
            got = flip(acc[14][lo:hi], bit)
            acc[m] = acc[m].at[lo:hi].set((wide(acc[m][lo:hi]) + wide(got)).astype(BF16))
        for m, src, bit in ((4, 12, 8), (2, 6, 4), (8, 10, 2)):
            acc[m] = (wide(acc[m]) + wide(flip(acc[src], bit))).astype(BF16)
        total = wide(acc[0])
        for bit in (8, 4, 2):
            total = total + wide(flip(acc[bit], bit))
        moe_out = total[:, :dim].astype(BF16)

        d_gate = jnp.sum(jnp.where(expert_hot, d_gate_e[:, None, :], 0.0), axis=2)
        d_picked = gate_w * (d_gate - jnp.sum(gate_w * d_gate, axis=1, keepdims=True))
        d_logits = jnp.sum(jnp.where(expert_hot, d_picked[:, :, None], 0.0), axis=1)
        d_logits_b = d_logits.astype(BF16)
        d_x = total[:, dim:] + jnp.einsum('te,de->td', d_logits_b, w_router, preferred_element_type=F32)
        grad_w_router = lax.psum(jnp.einsum('td,te->de', x_loc, d_logits_b, preferred_element_type=F32), ('tp', 'ep'))
        grad_b_router = lax.psum(jnp.sum(d_logits, axis=0), ('tp', 'ep'))

        grad_w_gate_up = jnp.einsum('egd,fg->edf', gwgut.astype(BF16), perm, preferred_element_type=F32).astype(BF16)
        gbgu = gbgu[:, 0]
        grad_b_gate_up = jnp.stack([gbgu[:, :width], gbgu[:, width:]], axis=2).reshape(n_exp, two_w)
        return (moe_out, d_x.astype(BF16), grad_w_gate_up, grad_b_gate_up, gwd.astype(BF16), gbd[:, 0], grad_w_router, grad_b_router)

    in_specs = (tok_spec, tok_spec, tok_spec, P(None, None), P(None), P('ep', None, 'tp'), P('ep', 'tp'), P('ep', 'tp', None), P('ep', None), tok_spec)
    out_specs = (tok_spec, tok_spec, P('ep', None, 'tp'), P('ep', 'tp'), P('ep', 'tp', None), P('ep', None), P(None, None), P(None))
    return jax.shard_map(device_fn, mesh=mesh, in_specs=in_specs, out_specs=out_specs, check_vma=False)
```

```python
import functools

import jax
import jax.numpy as jnp
from jax import lax
from jax.experimental import pallas as pl
from jax.experimental.pallas import tpu as pltpu
from jax.sharding import PartitionSpec as P

CLAMP_LIMIT = 7.0
SWIGLU_ALPHA = 1.702
BF16 = jnp.bfloat16
F32 = jnp.float32
CALLS = ((0, 1), (8, 9, 4, 5), (2, 3, 12, 13, 6, 7), (10, 11, 14, 15))
ORDER = sum(CALLS, ())


def clamped_swiglu(gate_raw, up_raw):
    gate_val = jnp.minimum(gate_raw, CLAMP_LIMIT)
    up_val = jnp.clip(up_raw, -CLAMP_LIMIT, CLAMP_LIMIT)
    return gate_val * jax.nn.sigmoid(SWIGLU_ALPHA * gate_val) * (up_val + 1.0)


def dot32(lhs, rhs):
    return jnp.dot(lhs, rhs, preferred_element_type=F32)


def expert_kernel(n_blocks, n_exp, tok, dim, width, chained, *refs):
    blocks = refs[:n_blocks]
    refs = refs[n_blocks:]
    wgu_hbm, wgut_hbm, wd_hbm, wdt_hbm, bgu_ref, bd_ref, selrow_ref, selcol_ref = refs[:8]
    refs = refs[8:]
    if chained:
        gwgut_in, gwd_in, gbgu_in, gbd_in = refs[:4]
        refs = refs[4:]
    outs = refs[:n_blocks]
    refs = refs[n_blocks:]
    dg_ref, gwgut_hbm, gwd_hbm, gbgu_ref, gbd_ref = refs[:5]
    (xd, out_buf, moe_acc, dx_acc, wgu, wgut, wd, wdt, gwgut, gwd, xe_s, de_s, dc_s, p_s, dr_s,
     in_sem, out_sem, w_sem, g_sem, a_sem) = refs[5:]
    meta_at = 2 * dim

    def load(i, buf):
        return pltpu.make_async_copy(blocks[i], xd.at[buf], in_sem.at[buf])

    def store(i, buf):
        return pltpu.make_async_copy(out_buf.at[buf], outs[i], out_sem.at[buf])

    def weights(e):
        return [pltpu.make_async_copy(src.at[e], dst.at[e], w_sem.at[k, e])
                for k, (src, dst) in enumerate(((wgu_hbm, wgu), (wgut_hbm, wgut), (wd_hbm, wd), (wdt_hbm, wdt)))]

    def sums_in(e):
        return [pltpu.make_async_copy(src.at[e], dst.at[e], a_sem.at[k, e])
                for k, (src, dst) in enumerate(((gwgut_in, gwgut), (gwd_in, gwd)))]

    def sums_out(e):
        return [pltpu.make_async_copy(src.at[e], dst.at[e], g_sem.at[k, e])
                for k, (src, dst) in enumerate(((gwgut, gwgut_hbm), (gwd, gwd_hbm)))]

    load(0, 0).start()
    for e in range(n_exp):
        for cp in weights(e) + (sums_in(e) if chained else []):
            cp.start()
    if chained:
        gbgu_ref[...] = gbgu_in[...]
        gbd_ref[...] = gbd_in[...]
    else:
        gwgut[...] = jnp.zeros_like(gwgut)
        gwd[...] = jnp.zeros_like(gwd)
        gbgu_ref[...] = jnp.zeros_like(gbgu_ref)
        gbd_ref[...] = jnp.zeros_like(gbd_ref)

    def step(it, carry):
        g = it // n_exp
        e = it % n_exp
        buf = g % 2

        @pl.when(e == 0)
        def _():
            for i in range(n_blocks):
                @pl.when(g == i)
                def _():
                    load(i, i % 2).wait()
                    if i + 1 < n_blocks:
                        load(i + 1, (i + 1) % 2).start()
                    if i >= 2:
                        store(i - 2, i % 2).wait()
            moe_acc[...] = jnp.zeros_like(moe_acc)
            dx_acc[...] = jnp.zeros_like(dx_acc)

        @pl.when(g == 0)
        def _():
            for k in range(n_exp):
                @pl.when(e == k)
                def _():
                    for cp in weights(k) + (sums_in(k) if chained else []):
                        cp.wait()

        meta = xd[buf, :, meta_at:meta_at + 128]
        rows = lax.dot_general(selrow_ref[e], meta, (((1,), (1,)), ((), ())), preferred_element_type=F32)
        slot_row = rows[0:1]
        w_row = rows[8:9]
        cols = dot32(meta, selcol_ref[e])
        slot_col = cols[:, :128].astype(jnp.int32)
        w_col = cols[:, 128:]
        count = jnp.max(slot_row)
        slot_i = slot_row.astype(jnp.int32)

        def tile(rows_t):
            hit = lax.broadcasted_iota(jnp.int32, (rows_t, tok), 0) == slot_i
            pick = jnp.where(hit, 1.0, 0.0).astype(BF16)
            w_slot = jnp.sum(jnp.where(hit, w_row, 0.0), axis=1, keepdims=True)
            sl = pl.ds(0, rows_t)
            for c in range(0, dim, 512):
                xe_s[sl, c:c + 512] = dot32(pick, xd[buf, :, c:c + 512]).astype(BF16)
            for c in range(0, dim, 512):
                d_rows = dot32(pick, xd[buf, :, dim + c:dim + c + 512])
                de_s[sl, c:c + 512] = d_rows
                dc_s[sl, c:c + 512] = (w_slot * d_rows).astype(BF16)
            hid = dot32(xe_s[sl, :], wgu[e]) + bgu_ref[e]
            act, pull = jax.vjp(clamped_swiglu, hid[:, :width], hid[:, width:])
            act_b = act.astype(BF16)
            dgs = jnp.zeros((rows_t, 1), F32)
            for c in range(0, dim, 512):
                part = (dot32(act_b, wd[e, :, c:c + 512]) + bd_ref[e, :, c:c + 512]).astype(BF16)
                p_s[sl, c:c + 512] = part
                dgs = dgs + jnp.sum(part.astype(F32) * de_s[sl, c:c + 512], axis=1, keepdims=True)
            dg_ref[it] = jnp.sum(jnp.where(hit, dgs, 0.0), axis=0, keepdims=True)
            d_act = dot32(dc_s[sl, :], wdt[e])
            d_gate, d_up = pull(d_act)
            d_hid = jnp.concatenate([d_gate, d_up], axis=1)
            gbgu_ref[e] += jnp.sum(d_hid, axis=0, keepdims=True)
            gbd_ref[e] += dot32(jnp.ones((16, rows_t), BF16), dc_s[sl, :])[0:1]
            d_hid_b = d_hid.astype(BF16)
            for c in range(0, dim, 512):
                dr_s[sl, c:c + 512] = dot32(d_hid_b, wgut[e, :, c:c + 512]).astype(BF16)
            act_t = act_b.T
            d_hid_t = d_hid_b.T
            for c in range(0, dim, 512):
                gwd[e, :, c:c + 512] += dot32(act_t, dc_s[sl, c:c + 512])
                gwgut[e, :, c:c + 512] += dot32(d_hid_t, xe_s[sl, c:c + 512])
            lane = lax.broadcasted_iota(jnp.int32, (tok, rows_t), 1)
            slot_wide = slot_col if rows_t == 128 else jnp.concatenate([slot_col] * (rows_t // 128), axis=1)
            place = jnp.where(lane == slot_wide, 1.0, 0.0).astype(BF16)
            w_wide = jnp.concatenate([w_col] * 4, axis=1)
            for c in range(0, dim, 512):
                moe_acc[:, c:c + 512] += w_wide * dot32(place, p_s[sl, c:c + 512])
                dx_acc[:, c:c + 512] += dot32(place, dr_s[sl, c:c + 512])

        @pl.when(count < 127.5)
        def _():
            tile(128)

        @pl.when(count > 127.5)
        def _():
            tile(256)

        @pl.when(g == n_blocks - 1)
        def _():
            for k in range(n_exp):
                @pl.when(e == k)
                def _():
                    for cp in sums_out(k):
                        cp.start()

        @pl.when(e == n_exp - 1)
        def _():
            out_buf[buf, :, :dim] = moe_acc[...].astype(BF16)
            out_buf[buf, :, dim:] = dx_acc[...].astype(BF16)
            for i in range(n_blocks):
                @pl.when(g == i)
                def _():
                    store(i, i % 2).start()
        return carry

    lax.fori_loop(0, n_blocks * n_exp, step, 0)
    for i in range(max(0, n_blocks - 2), n_blocks):
        store(i, i % 2).wait()
    for e in range(n_exp):
        for cp in sums_out(e):
            cp.wait()


def run_experts(blocks, weights, sums):
    wgu = weights[0]
    chained = sums is not None
    n_blocks = len(blocks)
    n_exp, dim, two_w = wgu.shape
    width = two_w // 2
    tok, row_w = blocks[0].shape
    any_spec = pl.BlockSpec(memory_space=pl.ANY)
    vm_spec = pl.BlockSpec(memory_space=pltpu.VMEM)
    flops = n_blocks * n_exp * 2 * 128 * dim * (6 * tok + 6 * two_w)
    out = pl.pallas_call(
        functools.partial(expert_kernel, n_blocks, n_exp, tok, dim, width, chained),
        out_shape=[jax.ShapeDtypeStruct((tok, 2 * dim), BF16)] * n_blocks + [
            jax.ShapeDtypeStruct((n_blocks * n_exp, 1, tok), F32),
            jax.ShapeDtypeStruct((n_exp, two_w, dim), F32),
            jax.ShapeDtypeStruct((n_exp, width, dim), F32),
            jax.ShapeDtypeStruct((n_exp, 1, two_w), F32),
            jax.ShapeDtypeStruct((n_exp, 1, dim), F32),
        ],
        in_specs=[any_spec] * (n_blocks + 4) + [vm_spec] * 4 + ([any_spec] * 2 + [vm_spec] * 2 if chained else []),
        out_specs=[any_spec] * n_blocks + [vm_spec, any_spec, any_spec, vm_spec, vm_spec],
        scratch_shapes=[
            pltpu.VMEM((2, tok, row_w), BF16),
            pltpu.VMEM((2, tok, 2 * dim), BF16),
            pltpu.VMEM((tok, dim), F32),
            pltpu.VMEM((tok, dim), F32),
            pltpu.VMEM((n_exp, dim, two_w), BF16),
            pltpu.VMEM((n_exp, two_w, dim), BF16),
            pltpu.VMEM((n_exp, width, dim), BF16),
            pltpu.VMEM((n_exp, dim, width), BF16),
            pltpu.VMEM((n_exp, two_w, dim), F32),
            pltpu.VMEM((n_exp, width, dim), F32),
            pltpu.VMEM((256, dim), BF16),
            pltpu.VMEM((256, dim), F32),
            pltpu.VMEM((256, dim), BF16),
            pltpu.VMEM((256, dim), BF16),
            pltpu.VMEM((256, dim), BF16),
            pltpu.SemaphoreType.DMA((2,)),
            pltpu.SemaphoreType.DMA((2,)),
            pltpu.SemaphoreType.DMA((4, n_exp)),
            pltpu.SemaphoreType.DMA((2, n_exp)),
            pltpu.SemaphoreType.DMA((2, n_exp)),
        ],
        compiler_params=pltpu.CompilerParams(vmem_limit_bytes=60 * 1024 * 1024),
        cost_estimate=pl.CostEstimate(flops=flops, bytes_accessed=n_blocks * tok * 4 * dim * 2, transcendentals=0),
        name='experts',
    )(*blocks, *weights, *(sums if chained else ()))
    return out[:n_blocks], out[n_blocks], list(out[n_blocks + 1:])


def solution(mesh):
    tp_count = mesh.shape['tp']
    ep_count = mesh.shape['ep']
    n_dev = tp_count * ep_count
    tok_spec = P(('ep', 'tp'), None)
    axes = ('tp', 'ep')

    def flip(val, bit):
        return lax.ppermute(val, axes, [(i, i ^ bit) for i in range(n_dev)])

    def device_fn(x_loc, idx_loc, slot_loc, w_router, b_router, w_gate_up, b_gate_up, w_down, b_down, dy_loc):
        tok, dim = x_loc.shape
        n_experts = w_router.shape[1]
        n_exp = w_gate_up.shape[0]
        two_w = w_gate_up.shape[2]
        width = two_w // 2
        tp_index = lax.axis_index('tp')
        ep_index = lax.axis_index('ep')
        cut = (0, 176, 352, tok)

        logits = dot32(x_loc, w_router) + b_router[None, :]
        expert_hot = idx_loc[:, :, None] == jnp.arange(n_experts)[None, None, :]
        picked = jnp.sum(jnp.where(expert_hot, logits[:, None, :], 0.0), axis=2)
        gate_w = jax.nn.softmax(picked, axis=1)
        kept = jnp.any(expert_hot & (slot_loc >= 0)[:, :, None], axis=1)
        before = (jnp.arange(tok)[:, None] > jnp.arange(tok)[None, :]).astype(BF16)
        rank = dot32(before, kept.astype(BF16))
        slot_e = jnp.where(kept, rank, -1.0)
        w_e = jnp.sum(jnp.where(expert_hot, gate_w[:, :, None], 0.0), axis=1)
        w_hi = lax.reduce_precision(w_e, 8, 7)
        w_mid = lax.reduce_precision(w_e - w_hi, 8, 7)
        w_lo = w_e - w_hi - w_mid
        meta = jnp.concatenate([slot_e, w_hi, w_mid, w_lo], axis=1).astype(BF16)
        own = jnp.concatenate([x_loc, dy_loc, meta], axis=1)

        blk = {0: own}
        for bit in (8, 4, 2):
            blk[bit] = flip(own, bit)
        blk[1] = flip(own, 1)

        col = jnp.arange(two_w)
        target = jnp.where(col % 2 == 0, col // 2, width + col // 2)
        perm = (target[:, None] == col[None, :]).astype(BF16)
        wgu = dot32(w_gate_up.reshape(n_exp * dim, two_w), perm).astype(BF16).reshape(n_exp, dim, two_w)
        wgut = jnp.swapaxes(wgu, 1, 2)
        wdt = jnp.swapaxes(w_down, 1, 2)
        bgu = b_gate_up.reshape(n_exp, width, 2)
        bgu = jnp.concatenate([bgu[:, :, 0], bgu[:, :, 1]], axis=1)[:, None, :]
        bias_on = (tp_index == 0).astype(F32)
        bd = (bias_on * b_down)[:, None, :]
        mine = ep_index * n_exp + jnp.arange(n_exp)
        lane = jnp.arange(128)
        sel_slot = lane[None, :] == mine[:, None]
        sel_w = (lane[None, :] % n_experts == mine[:, None]) & (lane[None, :] >= n_experts)
        row_id = jnp.arange(16)[None, :, None]
        selrow = jnp.where(row_id == 0, sel_slot[:, None, :], (row_id == 8) & sel_w[:, None, :]).astype(BF16)
        side = jnp.arange(256)[None, None, :] < 128
        selcol = jnp.where(side, sel_slot[:, :, None], sel_w[:, :, None]).astype(BF16)

        weights = (wgu, wgut, w_down, wdt, bgu, bd, selrow, selcol)
        part = {}
        dgs = []

        def experts(masks, sums):
            parts, dg, sums = run_experts([blk[m] for m in masks], weights, sums)
            part.update(zip(masks, parts))
            dgs.append(dg)
            return sums

        sums = experts(CALLS[0], None)
        blk[8], blk[4], blk[2], *sums = lax.optimization_barrier((blk[8], blk[4], blk[2], *sums))
        blk[12] = flip(blk[4], 8)
        blk[6] = flip(blk[2], 4)
        blk[10] = flip(blk[8], 2)
        for m in (8, 4, 2):
            blk[m + 1] = flip(blk[m], 1)
        sums = experts(CALLS[1], sums)
        blk[12], blk[6], blk[10], *sums = lax.optimization_barrier((blk[12], blk[6], blk[10], *sums))
        far = ((6, 8), (10, 4), (12, 2))
        thirds = [flip(blk[m][cut[k]:cut[k + 1]], bit) for k, (m, bit) in enumerate(far)]
        for m in (12, 6, 10):
            blk[m + 1] = flip(blk[m], 1)
        sums = experts(CALLS[2], sums)
        *thirds, sums[0] = lax.optimization_barrier((*thirds, sums[0]))
        blk[14] = jnp.concatenate(thirds, axis=0)
        blk[15] = flip(blk[14], 1)
        sums = experts(CALLS[3], sums)
        gwgut, gwd, gbgu, gbd = sums
        dg = jnp.concatenate([v.reshape(-1, n_exp * tok) for v in dgs], axis=0)
        lin = tp_index * ep_count + ep_index
        dg_abs = dg[jnp.array([ORDER.index(m) for m in range(n_dev)])][jnp.arange(n_dev) ^ lin]
        dg_back = lax.all_to_all(dg_abs, axes, 0, 0, tiled=True)

        def wide(val):
            return val.astype(F32)

        acc = {m: (wide(part[m]) + wide(flip(part[m + 1], 1))).astype(BF16) for m in range(0, 16, 2)}
        for k, (m, bit) in enumerate(far):
            lo, hi = cut[k], cut[k + 1]
            got = flip(acc[14][lo:hi], bit)
            acc[m] = acc[m].at[lo:hi].set((wide(acc[m][lo:hi]) + wide(got)).astype(BF16))
        acc[12], acc[6], acc[10], dg_back = lax.optimization_barrier((acc[12], acc[6], acc[10], dg_back))
        d_gate_e = dg_back.reshape(tp_count, ep_count * n_exp, tok).sum(axis=0).T
        for m, src, bit in ((4, 12, 8), (2, 6, 4), (8, 10, 2)):
            acc[m] = (wide(acc[m]) + wide(flip(acc[src], bit))).astype(BF16)
        got = [acc[0]] + [flip(acc[bit], bit) for bit in (8, 4, 2)]
        moe_out = sum(wide(v[:, :dim]) for v in got).astype(BF16)

        d_gate = jnp.sum(jnp.where(expert_hot, d_gate_e[:, None, :], 0.0), axis=2)
        d_picked = gate_w * (d_gate - jnp.sum(gate_w * d_gate, axis=1, keepdims=True))
        d_logits = jnp.sum(jnp.where(expert_hot, d_picked[:, :, None], 0.0), axis=1)
        d_logits_b = d_logits.astype(BF16)
        d_x = sum(wide(v[:, dim:]) for v in got) + jnp.einsum('te,de->td', d_logits_b, w_router, preferred_element_type=F32)
        g_router = jnp.einsum('te,td->ed', d_logits_b, x_loc, preferred_element_type=F32)
        g_bias = jnp.broadcast_to(jnp.sum(d_logits, axis=0)[:, None], (n_experts, 128))
        g_all = jnp.concatenate([g_router, g_bias], axis=1)
        for bit in (1, 8, 4, 2):
            g_all = g_all + flip(g_all, bit)
        grad_w_router = g_all[:, :dim].T
        grad_b_router = g_all[:, dim]

        grad_w_gate_up = jnp.einsum('egd,fg->edf', gwgut.astype(BF16), perm, preferred_element_type=F32).astype(BF16)
        gbgu = gbgu[:, 0]
        grad_b_gate_up = jnp.stack([gbgu[:, :width], gbgu[:, width:]], axis=2).reshape(n_exp, two_w)
        return (moe_out, d_x.astype(BF16), grad_w_gate_up, grad_b_gate_up, gwd.astype(BF16), gbd[:, 0], grad_w_router, grad_b_router)

    in_specs = (tok_spec, tok_spec, tok_spec, P(None, None), P(None), P('ep', None, 'tp'), P('ep', 'tp'), P('ep', 'tp', None), P('ep', None), tok_spec)
    out_specs = (tok_spec, tok_spec, P('ep', None, 'tp'), P('ep', 'tp'), P('ep', 'tp', None), P('ep', None), P(None, None), P(None))
    return jax.shard_map(device_fn, mesh=mesh, in_specs=in_specs, out_specs=out_specs, check_vma=False)
```

```python
import functools

import jax
import jax.numpy as jnp
from jax import lax
from jax.experimental import pallas as pl
from jax.experimental.pallas import tpu as pltpu
from jax.sharding import PartitionSpec as P

CLAMP_LIMIT = 7.0
SWIGLU_ALPHA = 1.702
BF16 = jnp.bfloat16
F32 = jnp.float32
CALLS = ((0, 1), (8, 9, 4, 5), (2, 3, 12, 13, 6, 7), (10, 11, 14, 15))
ORDER = sum(CALLS, ())


def clamped_swiglu(gate_raw, up_raw):
    gate_val = jnp.minimum(gate_raw, CLAMP_LIMIT)
    up_val = jnp.clip(up_raw, -CLAMP_LIMIT, CLAMP_LIMIT)
    return gate_val * jax.nn.sigmoid(SWIGLU_ALPHA * gate_val) * (up_val + 1.0)


def dot32(lhs, rhs):
    return jnp.dot(lhs, rhs, preferred_element_type=F32)


def expert_kernel(n_pairs, n_exp, tok, dim, width, *refs):
    n_blocks = 2 * n_pairs
    half = 128
    blocks = refs[:n_blocks]
    wgu_hbm, wgut_hbm, wd_hbm, wdt_hbm, bgu_ref, bd_ref, selrow_ref, selcol_ref = refs[n_blocks:n_blocks + 8]
    refs = refs[n_blocks + 8:]
    outs = refs[:n_blocks]
    dg_ref, gwgut_hbm, gwd_hbm, gbgu_ref, gbd_ref = refs[n_blocks:n_blocks + 5]
    (xd, out_buf, acc, wgu, wgut, wd, wdt, gwgut, gwd, rows_s, pick_s, wsl_s, xe_s, de_s, dc_s, hi_s, lo_s, dr_s,
     in_sem, out_sem, w_sem, g_sem) = refs[n_blocks + 5:]
    meta_at = 2 * dim

    def load(p, buf):
        return [pltpu.make_async_copy(blocks[2 * p + b], xd.at[buf, b], in_sem.at[buf, b]) for b in range(2)]

    def store(p, b):
        return pltpu.make_async_copy(out_buf.at[b], outs[2 * p + b], out_sem.at[b])

    def weights(e):
        return [pltpu.make_async_copy(src.at[e], dst.at[e], w_sem.at[k, e])
                for k, (src, dst) in enumerate(((wgu_hbm, wgu), (wgut_hbm, wgut), (wd_hbm, wd), (wdt_hbm, wdt)))]

    def sums_out(e):
        return [pltpu.make_async_copy(src.at[e], dst.at[e], g_sem.at[k, e])
                for k, (src, dst) in enumerate(((gwgut, gwgut_hbm), (gwd, gwd_hbm)))]

    for cp in load(0, 0):
        cp.start()
    for e in range(n_exp):
        for cp in weights(e):
            cp.start()
    gwgut[...] = jnp.zeros_like(gwgut)
    gwd[...] = jnp.zeros_like(gwd)
    gbgu_ref[...] = jnp.zeros_like(gbgu_ref)
    gbd_ref[...] = jnp.zeros_like(gbd_ref)

    def pair_step(p, carry):
        buf = p % 2
        for i in range(n_pairs):
            @pl.when(p == i)
            def _():
                for cp in load(i, i % 2):
                    cp.wait()
                if i + 1 < n_pairs:
                    for cp in load(i + 1, (i + 1) % 2):
                        cp.start()

        def gather(b, carry):
            at = pl.ds(pl.multiple_of(b * half, half), half)
            meta = xd[buf, b, :, meta_at:meta_at + 128]
            rows = lax.dot_general(selrow_ref[...], meta, (((1,), (1,)), ((), ())), preferred_element_type=F32)
            rows_s[b] = rows
            row_id = lax.broadcasted_iota(jnp.int32, (half, tok), 0).astype(F32)
            for e in range(n_exp):
                hit = row_id == rows[e:e + 1]
                pick_s[e * half:(e + 1) * half, :] = jnp.where(hit, 1.0, 0.0).astype(BF16)
                wsl_s[e, at, :] = jnp.sum(jnp.where(hit, rows[8 + e:9 + e], 0.0), axis=1, keepdims=True)
            for c in range(0, dim, 512):
                got = dot32(pick_s[...], xd[buf, b, :, c:c + 512]).astype(BF16)
                for e in range(n_exp):
                    xe_s[e, at, c:c + 512] = got[e * half:(e + 1) * half]
            for c in range(0, dim, 512):
                got = dot32(pick_s[...], xd[buf, b, :, dim + c:dim + c + 512]).astype(BF16)
                for e in range(n_exp):
                    de_s[e, at, c:c + 512] = got[e * half:(e + 1) * half]
            return carry

        lax.fori_loop(0, 2, gather, 0)

        def job(j, carry):
            e = j % n_exp
            over = j // n_exp
            base = over * half
            slots = [rows_s[b, pl.ds(e, 1), :] for b in range(2)]
            count = jnp.max(jnp.maximum(slots[0], slots[1]))

            @pl.when((p == 0) & (over == 0))
            def _():
                for k in range(n_exp):
                    @pl.when(e == k)
                    def _():
                        for cp in weights(k):
                            cp.wait()

            row_id = (lax.broadcasted_iota(jnp.int32, (half, tok), 0) + base).astype(F32)

            @pl.when((over == 1) & (count > 127.5))
            def _():
                for b in range(2):
                    hit = row_id == slots[b]
                    pick = jnp.where(hit, 1.0, 0.0).astype(BF16)
                    w_row = rows_s[b, pl.ds(8 + e, 1), :]
                    at = slice(b * half, (b + 1) * half)
                    wsl_s[e, at, :] = jnp.sum(jnp.where(hit, w_row, 0.0), axis=1, keepdims=True)
                    for c in range(0, dim, 512):
                        xe_s[e, at, c:c + 512] = dot32(pick, xd[buf, b, :, c:c + 512]).astype(BF16)
                        de_s[e, at, c:c + 512] = dot32(pick, xd[buf, b, :, dim + c:dim + c + 512]).astype(BF16)

            @pl.when((over == 0) | (count > 127.5))
            def _():
                w_slot = wsl_s[e]
                e_at = pl.ds(pl.multiple_of(e * half, half), half)
                for c in range(0, dim, 512):
                    dc_s[:, c:c + 512] = (w_slot * de_s[e, :, c:c + 512].astype(F32)).astype(BF16)
                hid = dot32(xe_s[e], wgu[e]) + bgu_ref[e]
                d_act = dot32(dc_s[...], wdt[e])
                act, pull = jax.vjp(clamped_swiglu, hid[:, :width], hid[:, width:])
                act_b = act.astype(BF16)
                d_gate, d_up = pull(d_act)
                d_hid = jnp.concatenate([d_gate, d_up], axis=1)
                gbgu_ref[e] += jnp.sum(d_hid, axis=0, keepdims=True)
                gbd_ref[e] += dot32(jnp.ones((16, 2 * half), BF16), dc_s[...])[0:1]
                d_hid_b = d_hid.astype(BF16)
                dgs = jnp.zeros((2 * half, 1), F32)
                for c in range(0, dim, 512):
                    part = (dot32(act_b, wd[e, :, c:c + 512]) + bd_ref[e, :, c:c + 512]).astype(BF16).astype(F32)
                    dgs = dgs + jnp.sum(part * de_s[e, :, c:c + 512].astype(F32), axis=1, keepdims=True)
                    wp = w_slot * part
                    hi = wp.astype(BF16)
                    lo = (wp - hi.astype(F32)).astype(BF16)
                    d_rows = dot32(d_hid_b, wgut[e, :, c:c + 512]).astype(BF16)
                    for b in range(2):
                        at = slice(b * half, (b + 1) * half)
                        hi_s[over, b, e_at, c:c + 512] = hi[at]
                        lo_s[over, b, e_at, c:c + 512] = lo[at]
                        dr_s[over, b, e_at, c:c + 512] = d_rows[at]
                for b in range(2):
                    hit = row_id == slots[b]
                    dg_row = jnp.sum(jnp.where(hit, dgs[b * half:(b + 1) * half], 0.0), axis=0, keepdims=True)
                    at = (2 * p + b) * n_exp + e
                    dg_ref[at] = dg_row + jnp.where(over == 0, 0.0, dg_ref[at])
                act_t = act_b.T
                d_hid_t = d_hid_b.T
                for c in range(0, dim, 512):
                    gwd[e, :, c:c + 512] += dot32(act_t, dc_s[:, c:c + 512])
                    gwgut[e, :, c:c + 512] += dot32(d_hid_t, xe_s[e, :, c:c + 512])

            @pl.when((p == n_pairs - 1) & (over == 1))
            def _():
                for k in range(n_exp):
                    @pl.when(e == k)
                    def _():
                        for cp in sums_out(k):
                            cp.start()
            return carry

        lax.fori_loop(0, 2 * n_exp, job, 0)

        for i in range(1, n_pairs):
            @pl.when(p == i)
            def _():
                for b in range(2):
                    store(i - 1, b).wait()

        def scatter(b, carry):
            meta = xd[buf, b, :, meta_at:meta_at + 128]
            lane = lax.broadcasted_iota(jnp.int32, (tok, half), 1).astype(F32)
            for e in range(n_exp):
                cols = dot32(meta, selcol_ref[e])
                pick_s[:, e * half:(e + 1) * half] = jnp.where(lane == cols, 1.0, 0.0).astype(BF16)
            place = pick_s
            spill = jnp.max(rows_s[b, 0:n_exp, :])

            def main(c):
                moe = dot32(place[...], hi_s[0, b, :, c:c + 512]) + dot32(place[...], lo_s[0, b, :, c:c + 512])
                return moe, dot32(place[...], dr_s[0, b, :, c:c + 512])

            @pl.when(spill < 127.5)
            def _():
                for c in range(0, dim, 512):
                    moe, d_x = main(c)
                    out_buf[b, :, c:c + 512] = moe.astype(BF16)
                    out_buf[b, :, dim + c:dim + c + 512] = d_x.astype(BF16)

            @pl.when(spill > 127.5)
            def _():
                for c in range(0, dim, 512):
                    moe, d_x = main(c)
                    acc[:, c:c + 512] = moe
                    acc[:, dim + c:dim + c + 512] = d_x

                def extra(e, carry):
                    @pl.when(jnp.max(rows_s[b, pl.ds(e, 1), :]) > 127.5)
                    def _():
                        cols = dot32(meta, selcol_ref[e])
                        put = jnp.where(lane + float(half) == cols, 1.0, 0.0).astype(BF16)
                        e_at = pl.ds(pl.multiple_of(e * half, half), half)
                        put2 = jnp.concatenate([put, put], axis=1)
                        for c in range(0, dim, 512):
                            both = jnp.concatenate([hi_s[1, b, e_at, c:c + 512], lo_s[1, b, e_at, c:c + 512]], axis=0)
                            acc[:, c:c + 512] += dot32(put2, both)
                            acc[:, dim + c:dim + c + 512] += dot32(put, dr_s[1, b, e_at, c:c + 512])
                    return carry

                lax.fori_loop(0, n_exp, extra, 0)
                for c in range(0, 2 * dim, 512):
                    out_buf[b, :, c:c + 512] = acc[:, c:c + 512].astype(BF16)
            return carry

        lax.fori_loop(0, 2, scatter, 0)
        for i in range(n_pairs):
            @pl.when(p == i)
            def _():
                for b in range(2):
                    store(i, b).start()
        return carry

    lax.fori_loop(0, n_pairs, pair_step, 0)
    for b in range(2):
        store(n_pairs - 1, b).wait()
    for e in range(n_exp):
        for cp in sums_out(e):
            cp.wait()


def run_experts(blocks, weights):
    wgu = weights[0]
    n_blocks = len(blocks)
    n_exp, dim, two_w = wgu.shape
    width = two_w // 2
    tok, row_w = blocks[0].shape
    any_spec = pl.BlockSpec(memory_space=pl.ANY)
    vm_spec = pl.BlockSpec(memory_space=pltpu.VMEM)
    flops = n_blocks * n_exp * 2 * 128 * dim * (6 * tok + 6 * two_w)
    out = pl.pallas_call(
        functools.partial(expert_kernel, n_blocks // 2, n_exp, tok, dim, width),
        out_shape=[jax.ShapeDtypeStruct((tok, 2 * dim), BF16)] * n_blocks + [
            jax.ShapeDtypeStruct((n_blocks * n_exp, 1, tok), F32),
            jax.ShapeDtypeStruct((n_exp, two_w, dim), F32),
            jax.ShapeDtypeStruct((n_exp, width, dim), F32),
            jax.ShapeDtypeStruct((n_exp, 1, two_w), F32),
            jax.ShapeDtypeStruct((n_exp, 1, dim), F32),
        ],
        in_specs=[any_spec] * (n_blocks + 4) + [vm_spec] * 4,
        out_specs=[any_spec] * n_blocks + [vm_spec, any_spec, any_spec, vm_spec, vm_spec],
        scratch_shapes=[
            pltpu.VMEM((2, 2, tok, row_w), BF16),
            pltpu.VMEM((2, tok, 2 * dim), BF16),
            pltpu.VMEM((tok, 2 * dim), F32),
            pltpu.VMEM((n_exp, dim, two_w), BF16),
            pltpu.VMEM((n_exp, two_w, dim), BF16),
            pltpu.VMEM((n_exp, width, dim), BF16),
            pltpu.VMEM((n_exp, dim, width), BF16),
            pltpu.VMEM((n_exp, two_w, dim), F32),
            pltpu.VMEM((n_exp, width, dim), F32),
            pltpu.VMEM((2, 16, tok), F32),
            pltpu.VMEM((tok, tok), BF16),
            pltpu.VMEM((n_exp, 256, 1), F32),
            pltpu.VMEM((n_exp, 256, dim), BF16),
            pltpu.VMEM((n_exp, 256, dim), BF16),
            pltpu.VMEM((256, dim), BF16),
            pltpu.VMEM((2, 2, n_exp * 128, dim), BF16),
            pltpu.VMEM((2, 2, n_exp * 128, dim), BF16),
            pltpu.VMEM((2, 2, n_exp * 128, dim), BF16),
            pltpu.SemaphoreType.DMA((2, 2)),
            pltpu.SemaphoreType.DMA((2,)),
            pltpu.SemaphoreType.DMA((4, n_exp)),
            pltpu.SemaphoreType.DMA((2, n_exp)),
        ],
        compiler_params=pltpu.CompilerParams(vmem_limit_bytes=63 * 1024 * 1024),
        cost_estimate=pl.CostEstimate(flops=flops, bytes_accessed=n_blocks * tok * 4 * dim * 2, transcendentals=0),
        name='experts',
    )(*blocks, *weights)
    return out[:n_blocks], out[n_blocks], list(out[n_blocks + 1:])


def solution(mesh):
    tp_count = mesh.shape['tp']
    ep_count = mesh.shape['ep']
    n_dev = tp_count * ep_count
    tok_spec = P(('ep', 'tp'), None)
    axes = ('tp', 'ep')

    def flip(val, bit):
        return lax.ppermute(val, axes, [(i, i ^ bit) for i in range(n_dev)])

    def device_fn(x_loc, idx_loc, slot_loc, w_router, b_router, w_gate_up, b_gate_up, w_down, b_down, dy_loc):
        tok, dim = x_loc.shape
        n_experts = w_router.shape[1]
        n_exp = w_gate_up.shape[0]
        two_w = w_gate_up.shape[2]
        width = two_w // 2
        tp_index = lax.axis_index('tp')
        ep_index = lax.axis_index('ep')
        cut = (0, 176, 352, tok)

        logits = dot32(x_loc, w_router) + b_router[None, :]
        expert_hot = idx_loc[:, :, None] == jnp.arange(n_experts)[None, None, :]
        picked = jnp.sum(jnp.where(expert_hot, logits[:, None, :], 0.0), axis=2)
        gate_w = jax.nn.softmax(picked, axis=1)
        kept = jnp.any(expert_hot & (slot_loc >= 0)[:, :, None], axis=1)
        before = (jnp.arange(tok)[:, None] > jnp.arange(tok)[None, :]).astype(BF16)
        rank = dot32(before, kept.astype(BF16))
        slot_e = jnp.where(kept, rank, -1.0)
        w_e = jnp.sum(jnp.where(expert_hot, gate_w[:, :, None], 0.0), axis=1)
        w_hi = lax.reduce_precision(w_e, 8, 7)
        w_mid = lax.reduce_precision(w_e - w_hi, 8, 7)
        w_lo = w_e - w_hi - w_mid
        meta = jnp.concatenate([slot_e, w_hi, w_mid, w_lo], axis=1).astype(BF16)
        own = jnp.concatenate([x_loc, dy_loc, meta], axis=1)

        blk = {0: own}
        for bit in (8, 4, 2):
            blk[bit] = flip(own, bit)
        blk[1] = flip(own, 1)

        col = jnp.arange(two_w)
        target = jnp.where(col % 2 == 0, col // 2, width + col // 2)
        perm = (target[:, None] == col[None, :]).astype(BF16)
        wgu = dot32(w_gate_up.reshape(n_exp * dim, two_w), perm).astype(BF16).reshape(n_exp, dim, two_w)
        wgut = jnp.swapaxes(wgu, 1, 2)
        wdt = jnp.swapaxes(w_down, 1, 2)
        bgu = b_gate_up.reshape(n_exp, width, 2)
        bgu = jnp.concatenate([bgu[:, :, 0], bgu[:, :, 1]], axis=1)[:, None, :]
        bias_on = (tp_index == 0).astype(F32)
        bd = (bias_on * b_down)[:, None, :]
        mine = ep_index * n_exp + jnp.arange(n_exp)
        lane = jnp.arange(128)
        sel_slot = lane[None, :] == mine[:, None]
        sel_w = (lane[None, :] % n_experts == mine[:, None]) & (lane[None, :] >= n_experts)
        blank = jnp.zeros((8 - n_exp, 128), bool)
        selrow = jnp.concatenate([sel_slot, blank, sel_w, blank], axis=0).astype(BF16)
        selcol = jnp.broadcast_to(sel_slot[:, :, None], (n_exp, 128, 128)).astype(BF16)

        weights = (wgu, wgut, w_down, wdt, bgu, bd)
        part = {}
        dgs = []

        def experts(masks):
            selrow_now, *dgs[-1:] = lax.optimization_barrier((selrow, *dgs[-1:]))
            parts, dg, sums = run_experts([blk[m] for m in masks], (*weights, selrow_now, selcol))
            part.update(zip(masks, parts))
            dgs.append(dg)
            all_sums.append(sums)

        all_sums = []
        experts(CALLS[0])
        blk[8], blk[4], blk[2], dgs[0] = lax.optimization_barrier((blk[8], blk[4], blk[2], dgs[0]))
        blk[12] = flip(blk[4], 8)
        blk[6] = flip(blk[2], 4)
        blk[10] = flip(blk[8], 2)
        for m in (8, 4, 2):
            blk[m + 1] = flip(blk[m], 1)
        experts(CALLS[1])
        blk[12], blk[6], blk[10], dgs[1] = lax.optimization_barrier((blk[12], blk[6], blk[10], dgs[1]))
        far = ((6, 8), (10, 4), (12, 2))
        thirds = [flip(blk[m][cut[k]:cut[k + 1]], bit) for k, (m, bit) in enumerate(far)]
        for m in (12, 6, 10):
            blk[m + 1] = flip(blk[m], 1)
        experts(CALLS[2])
        *thirds, dgs[2] = lax.optimization_barrier((*thirds, dgs[2]))
        blk[14] = jnp.concatenate(thirds, axis=0)
        blk[15] = flip(blk[14], 1)
        experts(CALLS[3])
        gwgut, gwd, gbgu, gbd = [functools.reduce(jnp.add, vals) for vals in zip(*all_sums)]
        dg = jnp.concatenate([v.reshape(-1, n_exp * tok) for v in dgs], axis=0)
        lin = tp_index * ep_count + ep_index
        dg_abs = dg[jnp.array([ORDER.index(m) for m in range(n_dev)])][jnp.arange(n_dev) ^ lin]
        dg_back = lax.all_to_all(dg_abs, axes, 0, 0, tiled=True)

        def wide(val):
            return val.astype(F32)

        acc = {m: (wide(part[m]) + wide(flip(part[m + 1], 1))).astype(BF16) for m in range(0, 16, 2)}
        for k, (m, bit) in enumerate(far):
            lo, hi = cut[k], cut[k + 1]
            got = flip(acc[14][lo:hi], bit)
            acc[m] = acc[m].at[lo:hi].set((wide(acc[m][lo:hi]) + wide(got)).astype(BF16))
        acc[12], acc[6], acc[10], dg_back = lax.optimization_barrier((acc[12], acc[6], acc[10], dg_back))
        d_gate_e = dg_back.reshape(tp_count, ep_count * n_exp, tok).sum(axis=0).T
        for m, src, bit in ((4, 12, 8), (2, 6, 4), (8, 10, 2)):
            acc[m] = (wide(acc[m]) + wide(flip(acc[src], bit))).astype(BF16)
        got = [acc[0]] + [flip(acc[bit], bit) for bit in (8, 4, 2)]
        moe_out = sum(wide(v[:, :dim]) for v in got).astype(BF16)

        d_gate = jnp.sum(jnp.where(expert_hot, d_gate_e[:, None, :], 0.0), axis=2)
        d_picked = gate_w * (d_gate - jnp.sum(gate_w * d_gate, axis=1, keepdims=True))
        d_logits = jnp.sum(jnp.where(expert_hot, d_picked[:, :, None], 0.0), axis=1)
        d_logits_b = d_logits.astype(BF16)
        d_x = sum(wide(v[:, dim:]) for v in got) + jnp.einsum('te,de->td', d_logits_b, w_router, preferred_element_type=F32)
        g_router = jnp.einsum('te,td->ed', d_logits_b, x_loc, preferred_element_type=F32)
        g_bias = jnp.broadcast_to(jnp.sum(d_logits, axis=0)[:, None], (n_experts, 128))
        g_all = jnp.concatenate([g_router, g_bias], axis=1)
        for bit in (1, 8, 4, 2):
            g_all = g_all + flip(g_all, bit)
        grad_w_router = g_all[:, :dim].T
        grad_b_router = g_all[:, dim]

        grad_w_gate_up = jnp.einsum('egd,fg->edf', gwgut.astype(BF16), perm, preferred_element_type=F32).astype(BF16)
        gbgu = gbgu[:, 0]
        grad_b_gate_up = jnp.stack([gbgu[:, :width], gbgu[:, width:]], axis=2).reshape(n_exp, two_w)
        return (moe_out, d_x.astype(BF16), grad_w_gate_up, grad_b_gate_up, gwd.astype(BF16), gbd[:, 0], grad_w_router, grad_b_router)

    in_specs = (tok_spec, tok_spec, tok_spec, P(None, None), P(None), P('ep', None, 'tp'), P('ep', 'tp'), P('ep', 'tp', None), P('ep', None), tok_spec)
    out_specs = (tok_spec, tok_spec, P('ep', None, 'tp'), P('ep', 'tp'), P('ep', 'tp', None), P('ep', None), P(None, None), P(None))
    return jax.shard_map(device_fn, mesh=mesh, in_specs=in_specs, out_specs=out_specs, check_vma=False)
```
